256 devices in a mesh: row: 8 (over y, core), col: 32 (over x, z).
Axes of the slice: x: 4, y: 4, z: 8, core: 2. Of those that a mesh axis runs over, the one named last changes fastest.
Arguments:
- sources: bfloat16 [8, 32, 4, 256, 256], P('row', 'col'), may hold values from -6 to 6
- history: bfloat16 [8, 32, 8, 256, 256], P(None, 'col'), may hold values from -4 to 4
- inverse_diagonal: float32 [8, 32, 256], P('row', 'col'), may hold values from 0.3 to 0.6
- far_cores: bfloat16 [8, 32, 32, 8, 32, 8, 32], P('row', None, None, None, 'col'), may hold values from -0.046875 to 0.046875
- target_basis: bfloat16 [8, 32, 256, 32], P('row', 'col'), may hold values from -1 to 1
- source_basis: bfloat16 [8, 32, 256, 32], P(None, 'col'), may hold values from -0.375 to 0.375
- near_blocks: bfloat16 [8, 32, 3, 256, 8, 256], P('row', 'col'), may hold values from -0.078125 to 0.078125
- near_tile: int32 [8, 32, 3], P('row', 'col'), may hold values from 0 to 7
- near_count: int32 [8, 32], P('row', 'col'), may hold values from 1 to 3, as said below
Outputs:
- new_steps: bfloat16 [8, 32, 4, 256, 256], P('row', 'col')
- energies: float32 [4, 256], replicated
The draws below stay inside these ranges and needn't reach their ends.
Inputs may be any that keep to these rules, and one draw needn't show every extreme that they name: Only slots below near_count are used; in every draw some tile has all 3 slots live.
All inputs are finite; a program needn't handle non-finite values.
Results may differ from the reference program's by a relative error of at most 0.011.
Values may be sent and summed in bfloat16 or wider, within the bound.
A program may use at most 192 MiB of HBM per device.

```python
import math
import jax
import jax.numpy as jnp
from jax import lax

TILE = 256
RANK = 32
LAGS = 8
STEPS = 4
SLOTS = 3
FIELDS = 256
PANELS = 65536
N_ROW = 8
N_COL = 32


def draw_near_count(key, part):
    first_key, other_key = jax.random.split(jax.random.fold_in(key, 7))
    counts = jax.random.randint(first_key, (N_ROW * N_COL,), 1, SLOTS + 1)
    chosen = jax.random.randint(other_key, (), 0, N_ROW * N_COL)
    counts = counts.at[chosen].set(SLOTS)
    return counts.reshape(N_ROW, N_COL).astype(jnp.int32)


def with_ends(values, own_key, smallest, largest):
    longest = values.shape.index(max(values.shape))
    spots = []
    for shift in (0, 1):
        where = [jax.random.randint(jax.random.fold_in(own_key, axis), (), 0, length) for axis, length in enumerate(values.shape)]
        where[longest] = (where[longest] + shift) % values.shape[longest]
        spots.append(tuple(where))
    return values.at[spots[0]].set(smallest).at[spots[1]].set(largest)


def strengthened(array, key, source, target, parts, factor):
    def block_of(position):
        return (jnp.arange(array.shape[position]) // (array.shape[position] // parts)).reshape((-1,) + (1,) * (array.ndim - 1 - position))

    first = jax.random.permutation(key, parts)[block_of(target)]
    second = (block_of(target) + parts // 2) % parts
    return jnp.where((block_of(source) == first) | (block_of(source) == second), factor * array, array)


def level_of(rng, shape, shards, smallest, top_value):
    def one(dim, blocks):
        draws = jax.random.uniform(jax.random.fold_in(jax.random.fold_in(rng, 6), dim), (blocks,), jnp.float32, smallest / len(shards), top_value / len(shards))
        return jnp.repeat(jnp.exp(draws), shape[dim] // blocks).reshape((-1,) + (1,) * (len(shape) - dim - 1))

    loudness = one(*shards[0])
    for cut in shards[1:]:
        loudness = loudness * one(*cut)
    return loudness


def noise(key, shape, spread, reach, cuts=(), held_as=jnp.bfloat16):
    factor_of = level_of(key, shape, cuts, -0.22, 0.18) if cuts else 1.0
    drawn = jax.random.normal(key, shape, jnp.float32) * spread * factor_of
    return jnp.minimum(jnp.maximum(drawn, -reach), reach).astype(held_as)


def noise_with(stream_key, shape, scale, limit, pieces, heavy, kind=jnp.bfloat16):
    result = scale * jax.random.normal(stream_key, shape, jnp.float32)
    if pieces:
        result = result * level_of(stream_key, shape, pieces, -0.22, 0.18)
    return jnp.clip(strengthened(result, jax.random.fold_in(stream_key, 3), *heavy), -limit, limit).astype(kind)


def setup_inputs(seed: int = 0) -> dict:
    seeds = jax.random.split(jax.random.key(seed), 10)
    return {
        "sources": noise(seeds[0], (N_ROW, N_COL, STEPS, TILE, FIELDS), 1.0, 6.0, ((0, 8), (1, 32))),
        "history": noise(seeds[1], (N_ROW, N_COL, LAGS, TILE, FIELDS), 0.5, 4.0, ((1, 32),)),
        "inverse_diagonal": jnp.clip(jnp.exp(math.log(0.6) - 0.6931472 * jax.random.uniform(seeds[2], (N_ROW, N_COL, TILE), jnp.float32) ** level_of(seeds[2], (N_ROW, N_COL, TILE), ((0, 8), (1, 32)), -0.2, 0.2)), 0.3, 0.6),
        "far_cores": noise_with(seeds[3], (N_ROW, N_COL, RANK, N_ROW, N_COL, LAGS, RANK), (N_ROW * N_COL * LAGS * RANK) ** -0.5, 0.046875, ((0, 8), (4, 32)), (4, 1, 32, 2.75)),
        "target_basis": noise(seeds[4], (N_ROW, N_COL, TILE, RANK), RANK ** -0.5, 1.0, ((0, 8), (1, 32))),
        "source_basis": noise(seeds[5], (N_ROW, N_COL, TILE, RANK), TILE ** -0.5, 0.375, ((1, 32),)),
        "near_blocks": noise(seeds[6], (N_ROW, N_COL, SLOTS, TILE, LAGS, TILE), (SLOTS * LAGS * TILE) ** -0.5, 0.078125, ((0, 8), (1, 32))),
        "near_tile": with_ends(jax.random.randint(seeds[7], (N_ROW, N_COL, SLOTS), 0, N_ROW), jax.random.fold_in(seeds[7], 1), 0, N_ROW - 1).astype(jnp.int32),
        "near_count": draw_near_count(jax.random.fold_in(seeds[9], 71), 0),
    }


def project(source_basis, blocks):
    return jnp.einsum("ijta,ijktx->ijkax", source_basis.astype(jnp.float32), blocks.astype(jnp.float32)).astype(jnp.bfloat16)


def reference(sources, history, inverse_diagonal, far_cores, target_basis, source_basis, near_blocks, near_tile, near_count):
    row_count = history.shape[0]
    col_count = history.shape[1]
    past = history
    projected = project(source_basis, past)
    flat_blocks = near_blocks.reshape(row_count * col_count, SLOTS, TILE, LAGS * TILE)
    flat_tiles = near_tile.reshape(row_count * col_count, SLOTS)
    flat_counts = near_count.reshape(row_count * col_count)
    col_ids = (jnp.arange(row_count * col_count, dtype=jnp.int32) % col_count).astype(jnp.int32)
    outputs = []
    energy_rows = []
    for moment in range(STEPS):
        stacked = projected.reshape(row_count * col_count * LAGS * RANK, FIELDS)

        def row_cores(cores_row):
            matrix = cores_row.reshape(col_count * RANK, row_count * col_count * LAGS * RANK)
            summed = jnp.dot(matrix, stacked, preferred_element_type=jnp.float32)
            return summed.astype(jnp.bfloat16).reshape(col_count, RANK, FIELDS)

        core_now = lax.map(row_cores, far_cores)
        far = jnp.einsum("ijta,ijax->ijtx", target_basis.astype(jnp.float32), core_now.astype(jnp.float32))

        def near_tile_sum(inputs):
            blocks, tiles, count, col_id = inputs
            column = lax.dynamic_index_in_dim(past, col_id, 1, keepdims=False)
            total = jnp.zeros((TILE, FIELDS), jnp.float32)
            for slot in range(SLOTS):
                source = lax.dynamic_index_in_dim(column, tiles[slot], 0, keepdims=False).reshape(LAGS * TILE, FIELDS)
                term = jnp.dot(blocks[slot], source, preferred_element_type=jnp.float32)
                total = total + jnp.where(slot < count, term, jnp.zeros_like(term))
            return total

        near = lax.map(near_tile_sum, (flat_blocks, flat_tiles, flat_counts, col_ids)).reshape(row_count, col_count, TILE, FIELDS)
        fresh = (inverse_diagonal[:, :, :, None] * (sources[:, :, moment].astype(jnp.float32) - far - near)).astype(jnp.bfloat16)
        outputs.append(fresh)
        energy_rows.append(jnp.sum(jnp.square(fresh.astype(jnp.float32)), axis=(0, 1, 2)) / PANELS)
        past = jnp.concatenate([fresh[:, :, None], past[:, :, :-1]], axis=2)
        projected = jnp.concatenate([project(source_basis, fresh[:, :, None]), projected[:, :, :-1]], axis=2)
    return jnp.stack(outputs, axis=2), jnp.stack(energy_rows, axis=0)
```

```python
import functools

import jax
import jax.numpy as jnp
from jax import lax
from jax.experimental import pallas as pl
from jax.experimental.pallas import tpu as pltpu
from jax.sharding import PartitionSpec as P

BF = jnp.bfloat16
F32 = jnp.float32
NX, NY, NZ, NC = 4, 4, 8, 2
ROWS, COLS = NY * NC, NX * NZ
TILE, RANK, LAGS, STEPS, SLOTS, FIELDS = 256, 32, 8, 4, 3, 256
XROWS = NZ * RANK
HALF = XROWS // 2
DEPTH = ROWS * RANK
PANELS = ROWS * COLS * TILE


def dot(a, b):
    return jnp.dot(a, b, preferred_element_type=F32)


def kernel(
    tile_ref, count_ref, inv_ref, tbt_ref, sbt_ref,
    src_hbm, hist_hbm, cores_hbm, near_hbm,
    out_hbm, en_ref,
    raw, cores, past, nraw, near, proj, new0, new1, new2, new3, early,
    src, scale, tbasis, nacc, sb2, sbp, sbm, r1, r2, sfull, sz, rz, er0, er1, er2,
    raw_sem, hist_sem, near_sem, src_sem, out_sem,
    ag_s, ag_r, ug_s, ug_r, x_s, x_r, z_s, z_r, e_s, e_r,
):
    row, col = lax.axis_index("row"), lax.axis_index("col")
    y, c = row // NC, lax.rem(row, NC)
    x, z = col // NZ, lax.rem(col, NZ)
    news = (new0, new1, new2, new3)

    def at_row(d):
        return (lax.rem(row + d, ROWS), col)

    def at_y(d):
        return (lax.rem(y + d, NY) * NC + c, col)

    def at_x(d):
        return (row, lax.rem(x + d, NX) * NZ + z)

    def at_z(d):
        return (row, x * NZ + lax.rem(z + d, NZ))

    partner = (y * NC + 1 - c, col)

    def send(a, b, s, r, dev):
        copy = pltpu.make_async_remote_copy(
            src_ref=a, dst_ref=b, send_sem=s, recv_sem=r, device_id=dev,
            device_id_type=pl.DeviceIdType.MESH,
        )
        copy.start()
        return copy

    barrier = pltpu.get_barrier_semaphore()
    peers = [at_row(d) for d in range(1, ROWS)]
    peers += [at_x(d) for d in range(1, NX)] + [at_z(d) for d in range(1, NZ)]
    for dev in peers:
        pl.semaphore_signal(barrier, inc=1, device_id=dev, device_id_type=pl.DeviceIdType.MESH)

    def raw_copy(j):
        return pltpu.make_async_copy(cores_hbm.at[0, j, :, :, 0], raw.at[j], raw_sem.at[j])

    def hist_copy(g):
        p, t = g // LAGS, lax.rem(g, LAGS)
        return pltpu.make_async_copy(
            hist_hbm.at[p, 0, LAGS - 1 - t],
            past.at[p, pl.ds(pl.multiple_of(t * TILE, TILE), TILE)],
            hist_sem.at[g],
        )

    per = ROWS * LAGS // COLS

    def start_loads(j, carry):
        raw_copy(j).start()
        for h in range(per):
            hist_copy(per * j + h).start()
        return carry

    lax.fori_loop(0, COLS, start_loads, 0)
    near_copies = [
        pltpu.make_async_copy(near_hbm.at[0, 0, s], nraw.at[s], near_sem.at[s]) for s in range(SLOTS)
    ]
    for copy in near_copies:
        copy.start()
    src_copy = pltpu.make_async_copy(src_hbm.at[0, 0], src, src_sem)
    src_copy.start()

    r_id = lax.broadcasted_iota(jnp.int32, (TILE, TILE), 0)
    c_id = lax.broadcasted_iota(jnp.int32, (TILE, TILE), 1)
    spread = jnp.where(r_id == c_id, jnp.broadcast_to(inv_ref[0], (TILE, TILE)), 0.0)
    scale[...] = jnp.broadcast_to(jnp.sum(spread, axis=1, keepdims=True), (TILE, FIELDS))
    tbasis[...] = jnp.transpose(tbt_ref[...].astype(F32)).astype(BF)

    def prepare(j, carry):
        raw_copy(j).wait()
        for h in range(per):
            hist_copy(per * j + h).wait()
        base = (j // NZ) * XROWS + lax.rem(j, NZ) * (RANK // 2)
        base = pl.multiple_of(base, RANK // 2)
        block = raw.at[j]
        group = 128 // RANK
        for h in range(ROWS // group):
            wide = jnp.concatenate(
                [block[:, group * h + q].astype(F32) for q in range(group)], axis=-1
            )
            turned = jnp.swapaxes(wide, 0, 1)
            for k in range(LAGS):
                piece = turned[k].astype(BF)
                lane = (LAGS - 1 - k) * DEPTH + h * 128
                cores[pl.ds(base, RANK // 2), lane : lane + 128] = piece[: RANK // 2]
                cores[pl.ds(base + HALF, RANK // 2), lane : lane + 128] = piece[RANK // 2 :]
        for h in range(per):
            g = per * j + h
            p, t = g // LAGS, lax.rem(g, LAGS)
            tile = past[p, pl.ds(pl.multiple_of(t * TILE, TILE), TILE), :]
            value = dot(sbt_ref[p], tile).astype(BF)
            proj[pl.ds(pl.multiple_of(t * DEPTH + p * RANK, RANK), RANK), :] = value
        return carry

    lax.fori_loop(0, COLS, prepare, 0)

    def prepare_near():
        for s in range(SLOTS):
            near_copies[s].wait()
            live = (s < count_ref[0, 0]).astype(F32)

            def turn(i, carry):
                r0 = pl.multiple_of(i * 32, 32)
                turned = jnp.swapaxes(nraw[s, pl.ds(r0, 32)].astype(F32), 0, 1) * live
                for k in range(LAGS):
                    lane = (LAGS - 1 - k) * TILE
                    near[s, pl.ds(r0, 32), lane : lane + TILE] = turned[k].astype(BF)
                return carry

            lax.fori_loop(0, TILE // 32, turn, 0)

    def near_old(n):
        depth = (LAGS - n) * TILE
        for s in range(SLOTS):
            tile = tile_ref[0, 0, s]
            total = dot(near[s, :, :depth], past[tile, n * TILE :, :])
            for r in range(n - 1):
                lane = (LAGS - n + r) * TILE
                total = total + dot(near[s, :, lane : lane + TILE], news[r][tile])
            nacc[...] = total if s == 0 else nacc[...] + total

    def near_last(n):
        lane = (LAGS - 1) * TILE
        total = nacc[...]
        for s in range(SLOTS):
            total = total + dot(near[s, :, lane : lane + TILE], news[n - 1][tile_ref[0, 0, s]])
        nacc[...] = total

    def early_rows(n, lo, hi):
        def one(i, carry):
            rows = pl.ds(pl.multiple_of(i * XROWS, XROWS), XROWS)
            depth = (LAGS - 1) * DEPTH
            early[n % 2, rows, :] = dot(
                cores[rows, :depth], proj[n * DEPTH : n * DEPTH + depth, :]
            )
            return carry

        lax.fori_loop(lo, hi, one, 0)

    pl.semaphore_wait(barrier, len(peers))

    sent = []
    ag = []
    ug = []
    outs = []
    for n in range(STEPS):
        if n:
            for copy in ag:
                copy.wait_recv()

        def block(d):
            rows = pl.ds(pl.multiple_of(lax.rem(x + d, NX) * XROWS, XROWS), XROWS)
            if n == 0:
                return rows, dot(cores[rows, :], proj[: LAGS * DEPTH, :])
            depth = (LAGS - 1) * DEPTH
            late = dot(cores[rows, depth:], proj[(n + LAGS - 1) * DEPTH : (n + LAGS) * DEPTH, :])
            return rows, early[n % 2, rows, :] + late

        def half(d, h):
            return pl.ds(pl.multiple_of(lax.rem(x + d, NX) * XROWS + h * HALF, HALF), HALF)

        lo, hi = slice(0, HALF), slice(HALF, XROWS)
        lo, hi = pl.ds(0, HALF), pl.ds(HALF, HALF)
        _, value = block(2)
        sb2[n] = value.astype(BF)
        c0 = send(sb2.at[n, lo], r1.at[n, 0], x_s.at[n, 0], x_r.at[n, 0], at_x(1))
        c1 = send(sb2.at[n, hi], r1.at[n, 1], x_s.at[n, 1], x_r.at[n, 1], at_x(3))
        rows, value = block(1)
        sbp[n, HALF:, :] = value[HALF:].astype(BF)
        early[n % 2, half(1, 0), :] = value[:HALF]
        c2 = send(sbp.at[n, hi], r2.at[n, 0, hi], x_s.at[n, 2], x_r.at[n, 2], at_x(1))
        rows, value = block(3)
        sbm[n, :HALF, :] = value[:HALF].astype(BF)
        early[n % 2, half(3, 1), :] = value[HALF:]
        c3 = send(sbm.at[n, lo], r2.at[n, 1, lo], x_s.at[n, 3], x_r.at[n, 3], at_x(3))
        rows, value = block(0)
        early[n % 2, rows, :] = value

        if n == 0:
            prepare_near()
        else:
            near_old(n)

        c0.wait_recv()
        sbp[n, :HALF, :] = (early[n % 2, half(1, 0), :] + r1[n, 0].astype(F32)).astype(BF)
        c4 = send(sbp.at[n, lo], r2.at[n, 0, lo], x_s.at[n, 4], x_r.at[n, 4], at_x(1))
        c1.wait_recv()
        sbm[n, HALF:, :] = (early[n % 2, half(3, 1), :] + r1[n, 1].astype(F32)).astype(BF)
        c5 = send(sbm.at[n, hi], r2.at[n, 1, hi], x_s.at[n, 5], x_r.at[n, 5], at_x(3))
        sent += [c0, c1, c2, c3, c4, c5]

        if n == 0:
            near_old(0)
        elif n + 1 < STEPS:
            early_rows(n + 1, 0, 2)

        for h, copies in ((0, (c3, c4)), (1, (c2, c5))):
            for copy in copies:
                copy.wait_recv()
            part = slice(h * HALF, (h + 1) * HALF)
            total = early[n % 2, half(0, h), :] + r2[n, 0, part, :].astype(F32)
            total = total + r2[n, 1, part, :].astype(F32)
            total = total.reshape(NZ, RANK // 2, FIELDS)
            lanes = slice(h * (RANK // 2), (h + 1) * (RANK // 2))
            sfull[:, lanes, :] = total
            sz[n, :, lanes, :] = total.astype(BF)
        zc = []
        for d in (4, 3, 5, 2, 6, 1, 7):
            zt = lax.rem(z + d, NZ)
            zc.append(
                send(sz.at[n, zt], rz.at[n, d], z_s.at[n, d - 1], z_r.at[n, d - 1], at_z(d))
            )
        sent += zc

        if n + 1 < STEPS:
            early_rows(n + 1, 0 if n == 0 else 2, NX)
        if n:
            for dy in range(1, NY):
                ug[dy - 1].wait_recv()
                got = lax.rem(y - dy + NY, NY) * NC + c
                ug.append(
                    send(
                        news[n - 1].at[got], news[n - 1].at[got],
                        ug_s.at[n - 1, 3 + dy], ug_r.at[n - 1, 3 + dy], partner,
                    )
                )
            for copy in ug[3:]:
                copy.wait_recv()
            sent += ug
            near_last(n)

        if n == 0:
            src_copy.wait()
        base = src[n].astype(F32) - nacc[...]
        nacc[...] = base
        for copy in zc:
            copy.wait_recv()
        core = sfull[z]
        for d in range(1, NZ):
            core = core + rz[n, d].astype(F32)
        far = dot(tbasis[...], core.astype(BF))
        fresh = (scale[...] * (nacc[...] - far)).astype(BF)
        dest = news[n].at[row] if n + 1 < STEPS else news[n]
        dest[...] = fresh
        if n + 1 < STEPS:
            mine = pl.ds(pl.multiple_of((LAGS + n) * DEPTH + row * RANK, RANK), RANK)
            proj[mine, :] = dot(sbt_ref[row], fresh).astype(BF)
            ag = [
                send(proj.at[mine], proj.at[mine], ag_s.at[n, d - 1], ag_r.at[n, d - 1], at_row(d))
                for d in (4, 3, 5, 2, 6, 1, 7)
            ]
            sent += ag
            ug = [
                send(dest, dest, ug_s.at[n, dy - 1], ug_r.at[n, dy - 1], at_y(dy))
                for dy in range(1, NY)
            ]
            ug.append(send(dest, dest, ug_s.at[n, 3], ug_r.at[n, 3], partner))
        wide = fresh.astype(F32)
        er0[row, n : n + 1, :] = jnp.sum(wide * wide, axis=0, keepdims=True) / PANELS
        out = pltpu.make_async_copy(dest, out_hbm.at[0, 0, n], out_sem.at[n])
        out.start()
        outs.append(out)

    def spread_sum(buf, mine, count, first, target):
        copies = [
            send(buf.at[mine], buf.at[mine], e_s.at[first + d - 1], e_r.at[first + d - 1], target(d))
            for d in range(1, count)
        ]
        for copy in copies:
            copy.wait_recv()
        total = buf[0]
        for i in range(1, count):
            total = total + buf[i]
        return total, copies

    total, copies = spread_sum(er0, row, ROWS, 0, at_row)
    sent += copies
    er1[x] = total
    total, copies = spread_sum(er1, x, NX, ROWS - 1, at_x)
    sent += copies
    er2[z] = total
    total, copies = spread_sum(er2, z, NZ, ROWS + NX - 2, at_z)
    sent += copies
    en_ref[...] = total
    for copy in sent:
        copy.wait_send()
    for copy in outs:
        copy.wait()


def local(
    sources, history, inverse_diagonal, far_cores, target_basis, source_basis,
    near_blocks, near_tile, near_count,
):
    smem = pl.BlockSpec(memory_space=pltpu.SMEM)
    vmem = pl.BlockSpec(memory_space=pltpu.VMEM)
    hbm = pl.BlockSpec(memory_space=pl.ANY)
    dma = pltpu.SemaphoreType.DMA
    tile = (TILE, FIELDS)
    new_steps, energies = pl.pallas_call(
        kernel,
        out_shape=(
            jax.ShapeDtypeStruct((1, 1, STEPS, *tile), BF),
            jax.ShapeDtypeStruct((STEPS, FIELDS), F32),
        ),
        in_specs=[smem, smem, vmem, vmem, vmem, hbm, hbm, hbm, hbm],
        out_specs=(hbm, vmem),
        scratch_shapes=[
            pltpu.VMEM((COLS, RANK, ROWS, LAGS, RANK), BF),
            pltpu.VMEM((COLS * RANK, LAGS * DEPTH), BF),
            pltpu.VMEM((ROWS, LAGS * TILE, FIELDS), BF),
            pltpu.VMEM((SLOTS, TILE, LAGS, TILE), BF),
            pltpu.VMEM((SLOTS, TILE, LAGS * TILE), BF),
            pltpu.VMEM(((LAGS + STEPS - 1) * DEPTH, FIELDS), BF),
            pltpu.VMEM((ROWS, *tile), BF),
            pltpu.VMEM((ROWS, *tile), BF),
            pltpu.VMEM((ROWS, *tile), BF),
            pltpu.VMEM(tile, BF),
            pltpu.VMEM((2, COLS * RANK, FIELDS), F32),
            pltpu.VMEM((STEPS, *tile), BF),
            pltpu.VMEM(tile, F32),
            pltpu.VMEM((TILE, RANK), BF),
            pltpu.VMEM(tile, F32),
            pltpu.VMEM((STEPS, XROWS, FIELDS), BF),
            pltpu.VMEM((STEPS, XROWS, FIELDS), BF),
            pltpu.VMEM((STEPS, XROWS, FIELDS), BF),
            pltpu.VMEM((STEPS, 2, HALF, FIELDS), BF),
            pltpu.VMEM((STEPS, 2, XROWS, FIELDS), BF),
            pltpu.VMEM((NZ, RANK, FIELDS), F32),
            pltpu.VMEM((STEPS, NZ, RANK, FIELDS), BF),
            pltpu.VMEM((STEPS, NZ, RANK, FIELDS), BF),
            pltpu.VMEM((ROWS, STEPS, FIELDS), F32),
            pltpu.VMEM((NX, STEPS, FIELDS), F32),
            pltpu.VMEM((NZ, STEPS, FIELDS), F32),
            dma((COLS,)), dma((ROWS * LAGS,)), dma((SLOTS,)), dma, dma((STEPS,)),
            dma((STEPS, 7)), dma((STEPS, 7)), dma((STEPS, 7)), dma((STEPS, 7)),
            dma((STEPS, 6)), dma((STEPS, 6)), dma((STEPS, 7)), dma((STEPS, 7)),
            dma((17,)), dma((17,)),
        ],
        compiler_params=pltpu.CompilerParams(
            collective_id=0, has_side_effects=True, vmem_limit_bytes=60 << 20
        ),
    )(
        near_tile, near_count, inverse_diagonal[0],
        jnp.swapaxes(target_basis, 2, 3)[0, 0], jnp.swapaxes(source_basis, 2, 3)[:, 0],
        sources, history, far_cores, near_blocks,
    )
    return new_steps, energies


def solution(mesh):
    placed = (
        P("row", "col", None, None, None),
        P(None, "col", None, None, None),
        P("row", "col", None),
        P("row", None, None, None, "col", None, None),
        P("row", "col", None, None),
        P(None, "col", None, None),
        P("row", "col", None, None, None, None),
        P("row", "col", None),
        P("row", "col"),
    )
    return jax.shard_map(
        local,
        mesh=mesh,
        in_specs=placed,
        out_specs=(P("row", "col", None, None, None), P()),
        check_vma=False,
    )
```
